8 devices in a mesh: dp: 2 (over z, y), sp: 4 (over x, core).
Axes of the slice: x: 2, y: 2, z: 1, core: 2. Of those that a mesh axis runs over, the one named last changes fastest.
Arguments:
- tok_in: bfloat16 [4096, 6144], P(('dp', 'sp')), parts along dimension 0
- tok_pos: int32 [4096], P(('dp', 'sp')), parts along dimension 0
- w_dq: bfloat16 [6144, 1536], replicated
- g_q: float32 [1536], replicated
- w_uq: bfloat16 [1536, 64, 192], replicated
- w_dkv: bfloat16 [6144, 576], replicated
- g_kv: float32 [512], replicated
- w_uk: bfloat16 [512, 64, 128], replicated
- w_uv: bfloat16 [512, 64, 128], replicated
- w_o: bfloat16 [64, 128, 6144], replicated
Outputs:
- output 1: bfloat16 [4096, 6144], P(('dp', 'sp')), parts along dimension 0
- output 2: bfloat16 [4096, 512], P(('dp', 'sp')), parts along dimension 0
- output 3: bfloat16 [4096, 64], P(('dp', 'sp')), parts along dimension 0
There are 2 independent parts. The reference program is written for one: setup_inputs(seed, part) draws one part's arguments, and reference() takes and returns one part's arrays. A program takes and returns all parts, laid end to end along the dimension named above; an argument that names none is the same for every part.
All inputs are finite; a program needn't handle non-finite values.
Results may differ from the reference program's by a relative error of at most 0.006.
Values are sent between devices in bfloat16 or wider.
A program may use at most 1 GiB of HBM per device.

```python
import math
import jax
import jax.numpy as jnp
from jax import lax

SEQ_LEN = 2048
ROW_BLOCK = 512
MODEL_DIM = 6144
NUM_HEADS = 64
Q_RANK = 1536
KV_RANK = 512
NOPE_DIM = 128
ROPE_DIM = 64
V_DIM = 128

ROPE_THETA = 10000.0
YARN_FACTOR = 40.0
ORIG_CTX = 4096.0
BETA_FAST = 32.0
BETA_SLOW = 1.0
NORM_EPS = 1e-6


def rope_freqs(rot_dim):
    half_dim = rot_dim // 2
    log_base = 2.0 * math.log(ROPE_THETA)
    low_idx = max(math.floor(rot_dim * math.log(ORIG_CTX / (BETA_FAST * 2.0 * math.pi)) / log_base), 0)
    high_idx = min(math.ceil(rot_dim * math.log(ORIG_CTX / (BETA_SLOW * 2.0 * math.pi)) / log_base), half_dim - 1)
    spread = max(high_idx - low_idx, 0.001)
    freq_list = []
    for freq_idx in range(half_dim):
        base_freq = ROPE_THETA ** (-2.0 * freq_idx / rot_dim)
        ramp_val = min(max((freq_idx - low_idx) / spread, 0.0), 1.0)
        freq_list.append(base_freq / YARN_FACTOR * ramp_val + base_freq * (1.0 - ramp_val))
    return jnp.asarray(freq_list, dtype=jnp.float32)


def rotate_half(act_in, cos_t, sin_t):
    half_dim = act_in.shape[-1] // 2
    first = act_in[..., :half_dim]
    second = act_in[..., half_dim:]
    return jnp.concatenate([first * cos_t - second * sin_t, second * cos_t + first * sin_t], axis=-1)


def rms_norm(act_in, gain):
    mean_sq = jnp.mean(act_in * act_in, axis=-1, keepdims=True)
    return act_in * lax.rsqrt(mean_sq + NORM_EPS) * gain


def setup_inputs(seed: int = 0, part: int = 0) -> dict:
    root_key = jax.random.key(seed)
    part_key = jax.random.fold_in(root_key, part)
    key_x, key_pos = jax.random.split(part_key)
    weight_keys = jax.random.split(root_key, 8)

    def draw_weight(sub_key, arr_shape, fan_in):
        return (jax.random.normal(sub_key, arr_shape, jnp.float32) * fan_in ** -0.5).astype(jnp.bfloat16)

    tok_in = jax.random.normal(key_x, (SEQ_LEN, MODEL_DIM), jnp.float32).astype(jnp.bfloat16)
    pos_steps = jax.random.randint(key_pos, (SEQ_LEN,), 1, 5, dtype=jnp.int32)
    tok_pos = (jnp.cumsum(pos_steps) - pos_steps[0]).astype(jnp.int32)
    w_dq = draw_weight(weight_keys[0], (MODEL_DIM, Q_RANK), MODEL_DIM)
    g_q = jax.random.uniform(weight_keys[1], (Q_RANK,), jnp.float32, 0.5, 1.5)
    w_uq = draw_weight(weight_keys[2], (Q_RANK, NUM_HEADS, NOPE_DIM + ROPE_DIM), Q_RANK)
    w_dkv = draw_weight(weight_keys[3], (MODEL_DIM, KV_RANK + ROPE_DIM), MODEL_DIM)
    g_kv = jax.random.uniform(weight_keys[4], (KV_RANK,), jnp.float32, 0.5, 1.5)
    w_uk = draw_weight(weight_keys[5], (KV_RANK, NUM_HEADS, NOPE_DIM), KV_RANK)
    w_uv = draw_weight(weight_keys[6], (KV_RANK, NUM_HEADS, V_DIM), KV_RANK)
    w_o = draw_weight(weight_keys[7], (NUM_HEADS, V_DIM, MODEL_DIM), NUM_HEADS * V_DIM)
    return dict(tok_in=tok_in, tok_pos=tok_pos, w_dq=w_dq, g_q=g_q, w_uq=w_uq, w_dkv=w_dkv, g_kv=g_kv, w_uk=w_uk, w_uv=w_uv, w_o=w_o)


def reference(tok_in, tok_pos, w_dq, g_q, w_uq, w_dkv, g_kv, w_uk, w_uv, w_o):
    qk_dim = NOPE_DIM + ROPE_DIM
    attn_scale = (0.1 * math.log(YARN_FACTOR) + 1.0) ** 2 / math.sqrt(qk_dim)
    angles = tok_pos.astype(jnp.float32)[:, None] * rope_freqs(ROPE_DIM)[None, :]
    cos_t = jnp.cos(angles)
    sin_t = jnp.sin(angles)
    q_lat = rms_norm(jnp.dot(tok_in, w_dq, preferred_element_type=jnp.float32), g_q).astype(jnp.bfloat16)
    q_full = jnp.dot(q_lat, w_uq.reshape(Q_RANK, NUM_HEADS * qk_dim), preferred_element_type=jnp.float32).reshape(SEQ_LEN, NUM_HEADS, qk_dim)
    q_nope = q_full[:, :, :NOPE_DIM].astype(jnp.bfloat16)
    q_rot = rotate_half(q_full[:, :, NOPE_DIM:], cos_t[:, None, :], sin_t[:, None, :]).astype(jnp.bfloat16)
    kv_lat = jnp.dot(tok_in, w_dkv, preferred_element_type=jnp.float32)
    cache_kv = rms_norm(kv_lat[:, :KV_RANK], g_kv).astype(jnp.bfloat16)
    cache_pe = rotate_half(kv_lat[:, KV_RANK:], cos_t, sin_t).astype(jnp.bfloat16)
    k_nope = jnp.dot(cache_kv, w_uk.reshape(KV_RANK, NUM_HEADS * NOPE_DIM), preferred_element_type=jnp.float32).reshape(SEQ_LEN, NUM_HEADS, NOPE_DIM).astype(jnp.bfloat16)
    values = jnp.dot(cache_kv, w_uv.reshape(KV_RANK, NUM_HEADS * V_DIM), preferred_element_type=jnp.float32).reshape(SEQ_LEN, NUM_HEADS, V_DIM).astype(jnp.bfloat16)
    key_idx = jnp.arange(SEQ_LEN)
    num_blocks = SEQ_LEN // ROW_BLOCK

    def head_attention(head_in):
        qn_head, qr_head, kn_head, v_head = head_in

        def block_attention(blk_idx):
            start = blk_idx * ROW_BLOCK
            qn_blk = lax.dynamic_slice_in_dim(qn_head, start, ROW_BLOCK, axis=0)
            qr_blk = lax.dynamic_slice_in_dim(qr_head, start, ROW_BLOCK, axis=0)
            logits = jnp.dot(qn_blk, kn_head.T, preferred_element_type=jnp.float32) + jnp.dot(qr_blk, cache_pe.T, preferred_element_type=jnp.float32)
            logits = logits * attn_scale
            row_idx = start + jnp.arange(ROW_BLOCK)
            logits = jnp.where(key_idx[None, :] <= row_idx[:, None], logits, -jnp.inf)
            attn_prob = jax.nn.softmax(logits, axis=-1).astype(jnp.bfloat16)
            return jnp.dot(attn_prob, v_head, preferred_element_type=jnp.float32).astype(jnp.bfloat16)

        return lax.map(block_attention, jnp.arange(num_blocks)).reshape(SEQ_LEN, V_DIM)

    head_outs = lax.map(head_attention, (jnp.swapaxes(q_nope, 0, 1), jnp.swapaxes(q_rot, 0, 1), jnp.swapaxes(k_nope, 0, 1), jnp.swapaxes(values, 0, 1)))
    attn_cat = jnp.swapaxes(head_outs, 0, 1).reshape(SEQ_LEN, NUM_HEADS * V_DIM)
    attn_out = jnp.dot(attn_cat, w_o.reshape(NUM_HEADS * V_DIM, MODEL_DIM), preferred_element_type=jnp.float32).astype(jnp.bfloat16)
    return attn_out, cache_kv, cache_pe
```

```python
import math
import jax
import jax.numpy as jnp
from jax import lax
from jax.experimental import pallas as pl
from jax.experimental.pallas import tpu as pltpu
from jax.sharding import PartitionSpec as P

ROPE_THETA = 10000.0
YARN_FACTOR = 40.0
ORIG_CTX = 4096.0
BETA_FAST = 32.0
BETA_SLOW = 1.0
NORM_EPS = 1e-6
BF = jnp.bfloat16
F32 = jnp.float32


def rope_freqs(rot_dim):
    half_dim = rot_dim // 2
    log_base = 2.0 * math.log(ROPE_THETA)
    low_idx = max(math.floor(rot_dim * math.log(ORIG_CTX / (BETA_FAST * 2.0 * math.pi)) / log_base), 0)
    high_idx = min(math.ceil(rot_dim * math.log(ORIG_CTX / (BETA_SLOW * 2.0 * math.pi)) / log_base), half_dim - 1)
    spread = max(high_idx - low_idx, 0.001)
    freq_list = []
    for freq_idx in range(half_dim):
        base_freq = ROPE_THETA ** (-2.0 * freq_idx / rot_dim)
        ramp_val = min(max((freq_idx - low_idx) / spread, 0.0), 1.0)
        freq_list.append(base_freq / YARN_FACTOR * ramp_val + base_freq * (1.0 - ramp_val))
    return jnp.asarray(freq_list, dtype=F32)


def attn_kernel(scale, info, wq, wk, wv, cq_m, cq_o, cs_m, cs_o, ckv, ckvt, pe, o_m, o_o, kbuf, vbuf, qbuf, sbuf, m_ref, l_ref, acc):
    me = info[0]
    n_pieces = info[1]
    rows = cq_m.shape[1]

    @pl.when(pl.program_id(0) == 0)
    def _():
        qbuf[:, :, 192:, :] = jnp.zeros_like(qbuf[:, :, 192:, :])

        @pl.loop(0, n_pieces)
        def _(c):
            slot = jnp.bitwise_and(me - c, 3)
            for h in range(2):
                kbuf[h, c, :, 128:] = pe[slot]

    for idx, (cq, cs) in enumerate(((cq_m, cs_m), (cq_o, cs_o))):
        cos, sin = cs[:32], cs[32:]
        u = jnp.dot(wq[...], cq[...], preferred_element_type=F32)
        for h in range(2):
            b = 192 * h
            z1, z2 = u[b + 128:b + 160], u[b + 160:b + 192]
            qbuf[idx, h, 0:128] = u[b:b + 128].astype(BF)
            qbuf[idx, h, 128:160] = (z1 * cos - z2 * sin).astype(BF)
            qbuf[idx, h, 160:192] = (z2 * cos + z1 * sin).astype(BF)

    wk2 = jnp.concatenate([wk[0], wk[1]], axis=1)
    wv2 = wv[...].reshape(256, wv.shape[2])

    @pl.loop(0, n_pieces)
    def _(c):
        slot = jnp.bitwise_and(me - c, 3)
        kn = jnp.dot(ckv[slot], wk2, preferred_element_type=F32).astype(BF)
        kbuf[0, c, :, :128] = kn[:, :128]
        kbuf[1, c, :, :128] = kn[:, 128:]
        vbuf[c] = jnp.dot(wv2, ckvt[slot], preferred_element_type=F32).astype(BF)

    def scores(idx, h, c):
        return jnp.dot(kbuf[h, c], qbuf[idx, h], preferred_element_type=F32)

    def absorb(h, c, s):
        m_old = m_ref[h]
        m_new = jnp.maximum(m_old, jnp.max(s, axis=0, keepdims=True))
        alpha = jnp.exp2((m_old - m_new) * scale)
        p = jnp.exp2((s - m_new) * scale)
        m_ref[h] = m_new
        l_ref[h] = l_ref[h] * alpha + jnp.sum(p.reshape(rows // 8, 8, rows), axis=0)
        acc[h] = acc[h] * alpha + jnp.dot(vbuf[c, 128 * h:128 * h + 128], p.astype(BF), preferred_element_type=F32)

    for idx, out in enumerate((o_m, o_o)):
        piece = info[2 + idx]
        m_ref[...] = jnp.full_like(m_ref, -jnp.inf)
        l_ref[...] = jnp.zeros_like(l_ref)
        acc[...] = jnp.zeros_like(acc)
        for h in range(2):
            sbuf[0, h] = scores(idx, h, 0)

        @pl.loop(0, piece)
        def _(j):
            now = jnp.bitwise_and(j, 1)
            for h in range(2):
                sbuf[1 - now, h] = scores(idx, h, j + 1)
            for h in range(2):
                absorb(h, j, sbuf[now, h])

        last = jnp.bitwise_and(piece, 1)
        keep = lax.broadcasted_iota(jnp.int32, (rows, rows), 0) <= lax.broadcasted_iota(jnp.int32, (rows, rows), 1)
        for h in range(2):
            absorb(h, piece, jnp.where(keep, sbuf[last, h], -jnp.inf))
            total = jnp.sum(l_ref[h], axis=0, keepdims=True)
            o_t = (acc[h] * (1.0 / total)).astype(BF)
            out[:, 128 * h:128 * h + 128] = o_t.T


def out_kernel(info, a, b, wa, wb, y):
    r = jnp.dot(a[...], wa[...], preferred_element_type=F32) + jnp.dot(b[...], wb[...], preferred_element_type=F32)
    y[...] = r.astype(BF)


def solution(mesh):
    groups = mesh.shape['sp']
    tok_spec = P(('dp', 'sp'))
    rows_spec = P(('dp', 'sp'), None)
    rep = P()

    def shift(x, k):
        return lax.ppermute(x, 'sp', [(i, (i + k) % groups) for i in range(groups)])

    def swap(x):
        return lax.ppermute(x, 'sp', [(i, i ^ 1) for i in range(groups)])

    def local_step(tok_in, tok_pos, w_dq, g_q, w_uq, w_dkv, g_kv, w_uk, w_uv, w_o):
        rows, width = tok_in.shape
        heads, qk_dim = w_uq.shape[1], w_uq.shape[2]
        q_rank, kv_rank = w_dq.shape[1], g_kv.shape[0]
        v_dim = w_uv.shape[2]
        rot = w_dkv.shape[1] - kv_rank
        half = rot // 2
        own = heads // 2
        pairs = own // 2
        scale = (0.1 * math.log(YARN_FACTOR) + 1.0) ** 2 / math.sqrt(qk_dim) * math.log2(math.e)
        me = lax.axis_index('sp')
        core = me % 2

        angles = tok_pos.astype(F32)[None, :] * rope_freqs(rot)[:, None]
        cs = jnp.concatenate([jnp.cos(angles), jnp.sin(angles)], axis=0)
        cos_t, sin_t = cs[:half].T, cs[half:].T
        kv = jnp.dot(tok_in, w_dkv, preferred_element_type=F32)
        a, b1, b2 = kv[:, :kv_rank], kv[:, kv_rank:kv_rank + half], kv[:, kv_rank + half:]
        cache_kv = (a * lax.rsqrt(jnp.mean(a * a, axis=-1, keepdims=True) + NORM_EPS) * g_kv).astype(BF)
        cache_pe = jnp.concatenate([b1 * cos_t - b2 * sin_t, b2 * cos_t + b1 * sin_t], axis=-1).astype(BF)
        lat = jnp.concatenate([cache_kv, cache_pe, jnp.zeros((rows, 128 - rot), BF)], axis=1)
        lats = jnp.stack([lat] + [shift(lat, k) for k in range(1, groups)])
        cs_o = swap(cs)

        uq = jnp.dot(tok_in, w_dq, preferred_element_type=F32)
        c_q = (uq * lax.rsqrt(jnp.mean(uq * uq, axis=-1, keepdims=True) + NORM_EPS) * g_q).astype(BF).T
        cq_o = swap(c_q)

        ckv = lats[:, :, :kv_rank]
        pe = lats[:, :, kv_rank:]
        ckvt = jnp.swapaxes(ckv, 1, 2)
        wq_t = jnp.transpose(w_uq, (1, 2, 0)).reshape(heads * qk_dim, q_rank)
        wk_h = jnp.transpose(lax.dynamic_slice_in_dim(w_uk, core * own, own, axis=1), (1, 0, 2))
        wv_h = jnp.transpose(lax.dynamic_slice_in_dim(w_uv, core * own, own, axis=1), (1, 2, 0))
        info = jnp.stack([me, 2 * (me // 2) + 2, me, me ^ 1, core]).astype(jnp.int32)
        full = pl.BlockSpec(memory_space=pltpu.VMEM)
        o_m, o_o = pl.pallas_call(
            lambda *r: attn_kernel(scale, *r),
            grid_spec=pltpu.PrefetchScalarGridSpec(
                num_scalar_prefetch=1,
                grid=(pairs,),
                in_specs=[
                    pl.BlockSpec((2 * qk_dim, q_rank), lambda p, i: (i[4] * pairs + p, 0)),
                    pl.BlockSpec((2, kv_rank, 128), lambda p, i: (p, 0, 0)),
                    pl.BlockSpec((2, 128, kv_rank), lambda p, i: (p, 0, 0)),
                ] + [full] * 7,
                out_specs=[pl.BlockSpec((rows, 2 * v_dim), lambda p, i: (0, p))] * 2,
                scratch_shapes=[
                    pltpu.VMEM((2, groups, rows, 256), BF),
                    pltpu.VMEM((groups, 2 * v_dim, rows), BF),
                    pltpu.VMEM((2, 2, 256, rows), BF),
                    pltpu.VMEM((2, 2, rows, rows), F32),
                    pltpu.VMEM((2, 1, rows), F32),
                    pltpu.VMEM((2, 8, rows), F32),
                    pltpu.VMEM((2, v_dim, rows), F32),
                ],
            ),
            out_shape=[jax.ShapeDtypeStruct((rows, own * v_dim), BF)] * 2,
            compiler_params=pltpu.CompilerParams(dimension_semantics=("arbitrary",), vmem_limit_bytes=56 << 20),
            cost_estimate=pl.CostEstimate(flops=90 * 10 ** 9, bytes_accessed=60 << 20, transcendentals=10 ** 8),
            name="attn",
        )(info, wq_t, wk_h, wv_h, c_q, cq_o, cs, cs_o, ckv, ckvt, pe)
        o_r = swap(o_o)
        bn = 512
        depth = own * v_dim
        attn_out = pl.pallas_call(
            out_kernel,
            grid_spec=pltpu.PrefetchScalarGridSpec(
                num_scalar_prefetch=1,
                grid=(width // bn,),
                in_specs=[full, full,
                          pl.BlockSpec((depth, bn), lambda n, i: (i[4], n)),
                          pl.BlockSpec((depth, bn), lambda n, i: (1 - i[4], n))],
                out_specs=pl.BlockSpec((rows, bn), lambda n, i: (0, n)),
            ),
            out_shape=jax.ShapeDtypeStruct((rows, width), BF),
            compiler_params=pltpu.CompilerParams(dimension_semantics=("arbitrary",), vmem_limit_bytes=56 << 20),
            cost_estimate=pl.CostEstimate(flops=52 * 10 ** 9, bytes_accessed=110 << 20, transcendentals=0),
            name="outproj",
        )(info, o_m, o_r, w_o.reshape(heads * v_dim, width), w_o.reshape(heads * v_dim, width))
        return attn_out, cache_kv, cache_pe

    return jax.shard_map(local_step, mesh=mesh, in_specs=(rows_spec, tok_spec) + (rep,) * 8, out_specs=(rows_spec,) * 3, check_vma=False)
```

```python
import math
import jax
import jax.numpy as jnp
from jax import lax
from jax.experimental import pallas as pl
from jax.experimental.pallas import tpu as pltpu
from jax.sharding import PartitionSpec as P

ROPE_THETA = 10000.0
YARN_FACTOR = 40.0
ORIG_CTX = 4096.0
BETA_FAST = 32.0
BETA_SLOW = 1.0
NORM_EPS = 1e-6
BF = jnp.bfloat16
F32 = jnp.float32


def rope_freqs(rot_dim):
    half_dim = rot_dim // 2
    log_base = 2.0 * math.log(ROPE_THETA)
    low_idx = max(math.floor(rot_dim * math.log(ORIG_CTX / (BETA_FAST * 2.0 * math.pi)) / log_base), 0)
    high_idx = min(math.ceil(rot_dim * math.log(ORIG_CTX / (BETA_SLOW * 2.0 * math.pi)) / log_base), half_dim - 1)
    spread = max(high_idx - low_idx, 0.001)
    freq_list = []
    for freq_idx in range(half_dim):
        base_freq = ROPE_THETA ** (-2.0 * freq_idx / rot_dim)
        ramp_val = min(max((freq_idx - low_idx) / spread, 0.0), 1.0)
        freq_list.append(base_freq / YARN_FACTOR * ramp_val + base_freq * (1.0 - ramp_val))
    return jnp.asarray(freq_list, dtype=F32)


def attn_kernel(scale, n_q, n_dep, info, *refs):
    wq, wk, wv = refs[:3]
    lats = refs[3:7]
    cqs = refs[7:7 + n_q]
    cs = refs[7 + n_q]
    o_m, o_o, ckv, cqv, kbuf, vbuf, qbuf, sbuf, m_ref, l_ref, acc, sems = refs[8 + n_q + n_dep:]
    me, n_pieces, p_m, p_o, skip, q_slot = (info[k] for k in range(6))
    rows = cqv.shape[2]
    step = pl.program_id(0)

    @pl.when(step == 0)
    def _():
        def fetch(base):
            return [pltpu.make_async_copy(cqs[base + k], cqv.at[k], sems.at[k]) for k in range(2)]

        for base in range(0, n_q, 2):
            @pl.when(q_slot == base)
            def _():
                for c in fetch(base):
                    c.start()
        copies = [pltpu.make_async_copy(lats[k], ckv.at[jnp.bitwise_xor(me, k)], sems.at[2 + k]) for k in range(4)]
        for c in copies:
            c.start()
        for c in copies + fetch(0):
            c.wait()
        qbuf[:, :, 192:, :] = jnp.zeros_like(qbuf[:, :, 192:, :])

        @pl.loop(0, n_pieces)
        def _(c):
            for h in range(2):
                kbuf[h, c, :, 128:] = ckv[c, :, 512:]

    def item(i):
        st = (i > p_m).astype(jnp.int32)
        return st, i - st * (p_m + 1)

    def qk(slot, st, c):
        for h in range(2):
            sbuf[slot, h] = jnp.dot(kbuf[h, c], qbuf[st, h], preferred_element_type=F32)

    def absorb(slot, st, c, masked):
        for h in range(2):
            s = sbuf[slot, h]
            if masked:
                keep = lax.broadcasted_iota(jnp.int32, (rows, rows), 0) <= lax.broadcasted_iota(jnp.int32, (rows, rows), 1)
                s = jnp.where(keep, s, -jnp.inf)
            m_old = m_ref[st, h]
            m_new = jnp.maximum(m_old, jnp.max(s, axis=0, keepdims=True))
            alpha = jnp.exp2((m_old - m_new) * scale)
            p = jnp.exp2((s - m_new) * scale)
            m_ref[st, h] = m_new
            l_ref[st, h] = l_ref[st, h] * alpha + jnp.sum(p.reshape(rows // 8, 8, rows), axis=0)
            acc[st, h] = acc[st, h] * alpha + jnp.dot(vbuf[c, 128 * h:128 * h + 128], p.astype(BF), preferred_element_type=F32)

    @pl.when(step >= skip)
    def _():
        @pl.loop(0, 2)
        def _(k):
            t = cs[q_slot + k]
            cos, sin = t[:32], t[32:]
            u = jnp.dot(wq[...], cqv[k], preferred_element_type=F32)
            for h in range(2):
                b = 192 * h
                z1, z2 = u[b + 128:b + 160], u[b + 160:b + 192]
                qbuf[k, h, 0:128] = u[b:b + 128].astype(BF)
                qbuf[k, h, 128:160] = (z1 * cos - z2 * sin).astype(BF)
                qbuf[k, h, 160:192] = (z2 * cos + z1 * sin).astype(BF)

        wkv = jnp.concatenate([wk[0], wk[1], wv[0], wv[1]], axis=1)

        @pl.loop(0, n_pieces)
        def _(c):
            kv = jnp.dot(ckv[c, :, :512], wkv, preferred_element_type=F32).astype(BF)
            kbuf[0, c, :, :128] = kv[:, :128]
            kbuf[1, c, :, :128] = kv[:, 128:256]
            vbuf[c] = kv[:, 256:].T

        m_ref[...] = jnp.full_like(m_ref, -jnp.inf)
        l_ref[...] = jnp.zeros_like(l_ref)
        acc[...] = jnp.zeros_like(acc)
        last = p_m + p_o + 1
        qk(0, 0, 0)

        @pl.loop(0, last)
        def _(i):
            now = jnp.bitwise_and(i, 1)
            st, c = item(i)
            st1, c1 = item(i + 1)
            diag = c == jnp.where(st == 0, p_m, p_o)

            def body(masked):
                qk(1 - now, st1, c1)
                absorb(now, st, c, masked)

            @pl.when(diag)
            def _():
                body(True)

            @pl.when(jnp.logical_not(diag))
            def _():
                body(False)

        absorb(jnp.bitwise_and(last, 1), 1, p_o, True)
        for st, out in ((0, o_m), (1, o_o)):
            for h in range(2):
                total = jnp.sum(l_ref[st, h], axis=0, keepdims=True)
                out[:, 128 * h:128 * h + 128] = (acc[st, h] * (1.0 / total)).astype(BF).T


def out_kernel(info, a_a, a_c, b_m, r_m, s_a, s_c, s_b, r_o, wa, wb, y, buf, sems):
    late = info[0] >= 2
    rows, seg = buf.shape[0] // 2, buf.shape[1] // 4

    def cols(ref, k):
        return ref.at[:, pl.ds(k * seg, seg)]

    @pl.when(pl.program_id(0) == 0)
    def _():
        def plan(is_late):
            mine = [cols(a_a, 1), b_m if is_late else cols(a_c, 0), cols(a_c, 1), r_m if is_late else cols(a_a, 0)]
            other = [cols(s_a, 1), s_b if is_late else cols(s_c, 0), cols(s_c, 1), r_o if is_late else cols(s_a, 0)]
            return [pltpu.make_async_copy(src, buf.at[pl.ds(g * rows, rows), pl.ds(k * seg, seg)], sems.at[4 * g + k])
                    for g, part in enumerate((mine, other)) for k, src in enumerate(part)]

        for is_late in (False, True):
            @pl.when(late == is_late)
            def _():
                for c in plan(is_late):
                    c.start()
        for c in plan(False):
            c.wait()

    half = rows // 2

    @pl.loop(0, 2)
    def _(k):
        r = jnp.dot(buf[pl.ds(k * half, half)], wa[...], preferred_element_type=F32) + jnp.dot(buf[pl.ds(rows + k * half, half)], wb[...], preferred_element_type=F32)
        y[pl.ds(k * half, half)] = r.astype(BF)


def solution(mesh):
    groups = mesh.shape['sp']
    tok_spec = P(('dp', 'sp'))
    rows_spec = P(('dp', 'sp'), None)
    rep = P()

    def xor(x, k, sources=range(4)):
        return lax.ppermute(x, 'sp', [(i, i ^ k) for i in sources])

    def run(tok_in, tok_pos, w_dq, g_q, w_uq, w_dkv, g_kv, w_uk, w_uv, w_o):
        rows, width = tok_in.shape
        heads, qk_dim = w_uq.shape[1], w_uq.shape[2]
        q_rank, kv_rank = w_dq.shape[1], g_kv.shape[0]
        v_dim = w_uv.shape[2]
        rot = w_dkv.shape[1] - kv_rank
        half = rot // 2
        own = heads // 2
        pairs = own // 2
        moved = 4
        scale = (0.1 * math.log(YARN_FACTOR) + 1.0) ** 2 / math.sqrt(qk_dim) * math.log2(math.e)
        me = lax.axis_index('sp')
        core = jnp.bitwise_and(me, 1)
        late = me >= 2

        pos = jnp.stack([tok_pos] + [xor(tok_pos, k) for k in range(1, 4)])
        angles = pos.astype(F32)[:, None, :] * rope_freqs(rot)[None, :, None]
        cs = jnp.concatenate([jnp.cos(angles), jnp.sin(angles)], axis=1)
        my_angles = tok_pos.astype(F32)[:, None] * rope_freqs(rot)[None, :]
        cos_t, sin_t = jnp.cos(my_angles), jnp.sin(my_angles)
        kv = jnp.dot(tok_in, w_dkv, preferred_element_type=F32)
        a, b1, b2 = kv[:, :kv_rank], kv[:, kv_rank:kv_rank + half], kv[:, kv_rank + half:]
        cache_kv = (a * lax.rsqrt(jnp.mean(a * a, axis=-1, keepdims=True) + NORM_EPS) * g_kv).astype(BF)
        cache_pe = jnp.concatenate([b1 * cos_t - b2 * sin_t, b2 * cos_t + b1 * sin_t], axis=-1).astype(BF)
        lat = jnp.concatenate([cache_kv, cache_pe, jnp.zeros((rows, 128 - rot), BF)], axis=1)
        lat_x = xor(lat, 2)
        lats = [lat, xor(lat, 1), lat_x, xor(lat_x, 1)]

        tok_in, lat = lax.optimization_barrier((tok_in, lat))
        uq = jnp.dot(tok_in, w_dq, preferred_element_type=F32)
        inv = lax.rsqrt(jnp.mean(uq * uq, axis=-1, keepdims=True) + NORM_EPS)
        c_q = (uq * inv * g_q).astype(BF).T
        cq_o = xor(c_q, 1)
        cq_x = xor(c_q, 2, (2, 3))
        cq_y = xor(c_q, 3, (2, 3))

        wq_t = jnp.transpose(w_uq, (1, 2, 0)).reshape(heads * qk_dim, q_rank)
        wk_h = jnp.transpose(lax.dynamic_slice_in_dim(w_uk, core * own, own, axis=1), (1, 0, 2))
        wv_h = jnp.transpose(lax.dynamic_slice_in_dim(w_uv, core * own, own, axis=1), (1, 0, 2))
        full = pl.BlockSpec(memory_space=pltpu.VMEM)
        hbm = pl.BlockSpec(memory_space=pl.ANY)

        def attend(steps, early_pair, late_pair, late_skip, foreign, *deps):
            pair0 = jnp.where(late, late_pair, early_pair)
            skip = jnp.where(late, late_skip, 0)
            if foreign:
                base = jnp.where(late, me, me ^ 2)
                pieces = jnp.full((), 4, jnp.int32)
                slot = jnp.where(late, 0, 2)
                cqs = [c_q, cq_o, cq_x, cq_y]
            else:
                base, pieces, slot = me, jnp.where(late, 4, 2), jnp.zeros((), jnp.int32)
                cqs = [c_q, cq_o]
            info = jnp.stack([me, pieces, base, base ^ 1, skip, slot, pair0, core]).astype(jnp.int32)

            def pair(p, i):
                return jnp.bitwise_and(i[6] + jnp.maximum(p, i[4]), pairs - 1)

            return pl.pallas_call(
                lambda *r: attn_kernel(scale, len(cqs), len(deps), *r),
                grid_spec=pltpu.PrefetchScalarGridSpec(
                    num_scalar_prefetch=1,
                    grid=(steps,),
                    in_specs=[
                        pl.BlockSpec((2 * qk_dim, q_rank), lambda p, i: (i[7] * pairs + pair(p, i), 0)),
                        pl.BlockSpec((2, kv_rank, v_dim), lambda p, i: (pair(p, i), 0, 0)),
                        pl.BlockSpec((2, kv_rank, v_dim), lambda p, i: (pair(p, i), 0, 0)),
                    ] + [hbm] * (4 + len(cqs)) + [full] + [hbm] * len(deps),
                    out_specs=[pl.BlockSpec((rows, 2 * v_dim), lambda p, i: (0, p))] * 2,
                    scratch_shapes=[
                        pltpu.VMEM((groups, rows, kv_rank + 128), BF),
                        pltpu.VMEM((2, q_rank, rows), BF),
                        pltpu.VMEM((2, groups, rows, 256), BF),
                        pltpu.VMEM((groups, 2 * v_dim, rows), BF),
                        pltpu.VMEM((2, 2, 256, rows), BF),
                        pltpu.VMEM((2, 2, rows, rows), F32),
                        pltpu.VMEM((2, 2, 1, rows), F32),
                        pltpu.VMEM((2, 2, 8, rows), F32),
                        pltpu.VMEM((2, 2, v_dim, rows), F32),
                        pltpu.SemaphoreType.DMA((6,)),
                    ],
                ),
                out_shape=[jax.ShapeDtypeStruct((rows, steps * 2 * v_dim), BF)] * 2,
                compiler_params=pltpu.CompilerParams(dimension_semantics=("arbitrary",), vmem_limit_bytes=48 << 20),
                cost_estimate=pl.CostEstimate(flops=5 * steps * 10 ** 9, bytes_accessed=2 * steps << 20, transcendentals=10 ** 7),
            )(info, wq_t, wk_h, wv_h, *lats, *cqs, cs, *deps)

        a_m, a_o = attend(8, pairs - moved, pairs - moved, moved, False)
        s_a = xor(a_o, 1)
        b_m, b_o = attend(moved, pairs - moved, 4, 0, True, a_m)
        r_m = xor(b_m, 2, (0, 1))
        r_o = xor(b_o, 3, (0, 1))
        s_b = xor(b_o, 1, (2, 3))
        c_m, c_o = attend(8, 4, 4, moved, False, b_m)
        s_c = xor(c_o, 1)
        bn = 512
        depth = own * v_dim
        info = jnp.stack([me, core]).astype(jnp.int32)
        w_o2 = w_o.reshape(heads * v_dim, width)
        attn_out = pl.pallas_call(
            out_kernel,
            grid_spec=pltpu.PrefetchScalarGridSpec(
                num_scalar_prefetch=1,
                grid=(width // bn,),
                in_specs=[hbm] * 8 + [
                    pl.BlockSpec((depth, bn), lambda n, i: (i[1], n)),
                    pl.BlockSpec((depth, bn), lambda n, i: (1 - i[1], n))],
                out_specs=pl.BlockSpec((rows, bn), lambda n, i: (0, n)),
                scratch_shapes=[pltpu.VMEM((2 * rows, depth), BF), pltpu.SemaphoreType.DMA((8,))],
            ),
            out_shape=jax.ShapeDtypeStruct((rows, width), BF),
            compiler_params=pltpu.CompilerParams(dimension_semantics=("arbitrary",), vmem_limit_bytes=56 << 20),
            cost_estimate=pl.CostEstimate(flops=52 * 10 ** 9, bytes_accessed=110 << 20, transcendentals=0),
            name="outproj",
        )(info, a_m, c_m, b_m, r_m, s_a, s_c, s_b, r_o, w_o2, w_o2)
        return attn_out, cache_kv, cache_pe

    return jax.shard_map(run, mesh=mesh, in_specs=(rows_spec, tok_spec) + (rep,) * 8, out_specs=(rows_spec,) * 3, check_vma=False)
```

```python
import math
import jax
import jax.numpy as jnp
from jax import lax
from jax.experimental import pallas as pl
from jax.experimental.pallas import tpu as pltpu
from jax.sharding import PartitionSpec as P

ROPE_THETA = 10000.0
YARN_FACTOR = 40.0
ORIG_CTX = 4096.0
BETA_FAST = 32.0
BETA_SLOW = 1.0
NORM_EPS = 1e-6
BF = jnp.bfloat16
F32 = jnp.float32


def rope_freqs(rot_dim):
    half_dim = rot_dim // 2
    log_base = 2.0 * math.log(ROPE_THETA)
    low_idx = max(math.floor(rot_dim * math.log(ORIG_CTX / (BETA_FAST * 2.0 * math.pi)) / log_base), 0)
    high_idx = min(math.ceil(rot_dim * math.log(ORIG_CTX / (BETA_SLOW * 2.0 * math.pi)) / log_base), half_dim - 1)
    spread = max(high_idx - low_idx, 0.001)
    freq_list = []
    for freq_idx in range(half_dim):
        base_freq = ROPE_THETA ** (-2.0 * freq_idx / rot_dim)
        ramp_val = min(max((freq_idx - low_idx) / spread, 0.0), 1.0)
        freq_list.append(base_freq / YARN_FACTOR * ramp_val + base_freq * (1.0 - ramp_val))
    return jnp.asarray(freq_list, dtype=F32)


def attn_kernel(scale, n_q, n_dep, info, *refs):
    wq, wk, wv = refs[:3]
    lats = refs[3:7]
    cqs = refs[7:7 + n_q]
    cs = refs[7 + n_q]
    o_m, o_o, ckv, cqv, kbuf, vbuf, qbuf, sbuf, m_ref, x_ref, l_ref, acc, obuf, sems = refs[8 + n_q + n_dep:]
    me, n_pieces, p_m, p_o, skip, q_slot = (info[k] for k in range(6))
    rows = cqv.shape[2]
    step = pl.program_id(0)

    @pl.when(step == 0)
    def _():
        def fetch(base):
            return [pltpu.make_async_copy(cqs[base + k], cqv.at[k], sems.at[k]) for k in range(2)]

        for base in range(0, n_q, 2):
            @pl.when(q_slot == base)
            def _():
                for c in fetch(base):
                    c.start()
        copies = [pltpu.make_async_copy(lats[k], ckv.at[jnp.bitwise_xor(me, k)], sems.at[2 + k]) for k in range(4)]
        for c in copies:
            c.start()
        for c in copies + fetch(0):
            c.wait()
        qbuf[:, :, 192:, :] = jnp.zeros_like(qbuf[:, :, 192:, :])

        @pl.loop(0, n_pieces)
        def _(c):
            for h in range(2):
                kbuf[h, c, :, 128:] = ckv[c, :, 512:]

    @pl.when(step >= skip)
    def _():
        @pl.loop(0, 2)
        def _(k):
            t = cs[q_slot + k]
            cos, sin = t[:32], t[32:]
            u = jnp.dot(wq[...], cqv[k], preferred_element_type=F32)
            for h in range(2):
                b = 192 * h
                z1, z2 = u[b + 128:b + 160], u[b + 160:b + 192]
                qbuf[k, h, 0:128] = u[b:b + 128].astype(BF)
                qbuf[k, h, 128:160] = (z1 * cos - z2 * sin).astype(BF)
                qbuf[k, h, 160:192] = (z2 * cos + z1 * sin).astype(BF)

        wkv = jnp.concatenate([wk[0], wk[1], wv[0], wv[1]], axis=1)

        @pl.loop(0, n_pieces)
        def _(c):
            kv = jnp.dot(ckv[c, :, :512], wkv, preferred_element_type=F32).astype(BF)
            kbuf[0, c, :, :128] = kv[:, :128]
            kbuf[1, c, :, :128] = kv[:, 128:256]
            vbuf[c] = kv[:, 256:].T

        @pl.loop(0, 2)
        def _(st):
            p_st = jnp.where(st == 0, p_m, p_o)
            m_ref[...] = jnp.full_like(m_ref, -jnp.inf)
            l_ref[...] = jnp.zeros_like(l_ref)
            acc[...] = jnp.zeros_like(acc)

            def first(c, h, masked):
                s = jnp.dot(kbuf[h, c], qbuf[st, h], preferred_element_type=F32)
                if masked:
                    keep = lax.broadcasted_iota(jnp.int32, (rows, rows), 0) <= lax.broadcasted_iota(jnp.int32, (rows, rows), 1)
                    s = jnp.where(keep, s, -jnp.inf)
                sbuf[c, h] = s
                m_ref[h] = jnp.maximum(m_ref[h], jnp.max(s.reshape(rows // 8, 8, rows), axis=0))

            def second(c, h):
                m = x_ref[h]
                p = jnp.exp2((sbuf[c, h] - m) * scale)
                l_ref[h] = l_ref[h] + jnp.sum(p.reshape(rows // 8, 8, rows), axis=0)
                acc[h] = acc[h] + jnp.dot(vbuf[c, pl.ds(128 * h, 128)], p.astype(BF), preferred_element_type=F32)

            def both(f):
                f(0)
                f(1)

            @pl.loop(0, p_st)
            def _(c):
                both(lambda h: first(c, h, False))

            both(lambda h: first(p_st, h, True))
            for h in range(2):
                x_ref[h] = jnp.max(m_ref[h], axis=0, keepdims=True)

            @pl.loop(0, p_st + 1)
            def _(c):
                both(lambda h: second(c, h))

            for h in range(2):
                total = jnp.sum(l_ref[h], axis=0, keepdims=True)
                obuf[st, h] = (acc[h] * (1.0 / total)).astype(BF).T

        for st, out in ((0, o_m), (1, o_o)):
            for h in range(2):
                out[:, 128 * h:128 * h + 128] = obuf[st, h]


def out_kernel(early, late, info, a_m, c_m, b_m, r_m, a_o, c_o, b_o, r_o, wa, wb, y, buf, sems):
    col = 256

    @pl.when(pl.program_id(0) == 0)
    def _():
        for is_late, runs in ((False, early), (True, late)):
            @pl.when((info[0] >= 2) == is_late)
            def _():
                copies = []
                for g, part in enumerate(((a_m, b_m, c_m, r_m), (a_o, b_o, c_o, r_o))):
                    for n, (src, first, count, place) in enumerate(runs):
                        copies.append(pltpu.make_async_copy(
                            part[src].at[:, pl.ds(first * col, count * col)],
                            buf.at[g, :, pl.ds(place * col, count * col)], sems.at[4 * g + n]))
                for c in copies:
                    c.start()
                for c in copies:
                    c.wait()

    r = jnp.dot(buf[0], wa[...], preferred_element_type=F32) + jnp.dot(buf[1], wb[...], preferred_element_type=F32)
    y[...] = r.astype(BF)


def solution(mesh):
    groups = mesh.shape['sp']
    tok_spec = P(('dp', 'sp'))
    rows_spec = P(('dp', 'sp'), None)
    rep = P()

    def xor(x, k, sources=range(4)):
        return lax.ppermute(x, 'sp', [(i, i ^ k) for i in sources])

    def run(tok_in, tok_pos, w_dq, g_q, w_uq, w_dkv, g_kv, w_uk, w_uv, w_o):
        rows, width = tok_in.shape
        heads, qk_dim = w_uq.shape[1], w_uq.shape[2]
        q_rank, kv_rank = w_dq.shape[1], g_kv.shape[0]
        v_dim = w_uv.shape[2]
        rot = w_dkv.shape[1] - kv_rank
        half = rot // 2
        own = heads // 2
        pairs = own // 2
        moved = 3
        scale = (0.1 * math.log(YARN_FACTOR) + 1.0) ** 2 / math.sqrt(qk_dim) * math.log2(math.e)
        me = lax.axis_index('sp')
        core = jnp.bitwise_and(me, 1)
        is_late = me >= 2

        pos = jnp.stack([tok_pos] + [xor(tok_pos, k) for k in range(1, 4)])
        angles = pos.astype(F32)[:, None, :] * rope_freqs(rot)[None, :, None]
        cs = jnp.concatenate([jnp.cos(angles), jnp.sin(angles)], axis=1)
        my_angles = tok_pos.astype(F32)[:, None] * rope_freqs(rot)[None, :]
        cos_t, sin_t = jnp.cos(my_angles), jnp.sin(my_angles)
        kv = jnp.dot(tok_in, w_dkv, preferred_element_type=F32)
        a, b1, b2 = kv[:, :kv_rank], kv[:, kv_rank:kv_rank + half], kv[:, kv_rank + half:]
        cache_kv = (a * lax.rsqrt(jnp.mean(a * a, axis=-1, keepdims=True) + NORM_EPS) * g_kv).astype(BF)
        cache_pe = jnp.concatenate([b1 * cos_t - b2 * sin_t, b2 * cos_t + b1 * sin_t], axis=-1).astype(BF)
        lat = jnp.concatenate([cache_kv, cache_pe, jnp.zeros((rows, 128 - rot), BF)], axis=1)
        lat_x = xor(lat, 2)
        lats = [lat, xor(lat, 1), lat_x, xor(lat_x, 1)]

        tok_in, lat = lax.optimization_barrier((tok_in, lat))
        uq = jnp.dot(tok_in, w_dq, preferred_element_type=F32)
        inv = lax.rsqrt(jnp.mean(uq * uq, axis=-1, keepdims=True) + NORM_EPS)
        c_q = (uq * inv * g_q).astype(BF).T
        cq_o = xor(c_q, 1)
        cq_x = xor(c_q, 2, (2, 3))
        cq_y = xor(cq_x, 1, (0, 1))

        wq_t = jnp.transpose(w_uq, (1, 2, 0)).reshape(heads * qk_dim, q_rank)
        wk_h = jnp.transpose(lax.dynamic_slice_in_dim(w_uk, core * own, own, axis=1), (1, 0, 2))
        wv_h = jnp.transpose(lax.dynamic_slice_in_dim(w_uv, core * own, own, axis=1), (1, 0, 2))
        full = pl.BlockSpec(memory_space=pltpu.VMEM)
        hbm = pl.BlockSpec(memory_space=pl.ANY)

        def attend(steps, early_pair, late_pair, late_skip, foreign, *deps):
            pair0 = jnp.where(is_late, late_pair, early_pair)
            skip = jnp.where(is_late, late_skip, 0)
            if foreign:
                base = jnp.where(is_late, me, me ^ 2)
                pieces = jnp.full((), 4, jnp.int32)
                slot = jnp.where(is_late, 0, 2)
                cqs = [c_q, cq_o, cq_x, cq_y]
            else:
                base, pieces, slot = me, jnp.where(is_late, 4, 2), jnp.zeros((), jnp.int32)
                cqs = [c_q, cq_o]
            info = jnp.stack([me, pieces, base, base ^ 1, skip, slot, pair0, core]).astype(jnp.int32)

            def pair(p, i):
                return jnp.bitwise_and(i[6] + jnp.maximum(p, i[4]), pairs - 1)

            return pl.pallas_call(
                lambda *r: attn_kernel(scale, len(cqs), len(deps), *r),
                grid_spec=pltpu.PrefetchScalarGridSpec(
                    num_scalar_prefetch=1,
                    grid=(steps,),
                    in_specs=[
                        pl.BlockSpec((2 * qk_dim, q_rank), lambda p, i: (i[7] * pairs + pair(p, i), 0)),
                        pl.BlockSpec((2, kv_rank, v_dim), lambda p, i: (pair(p, i), 0, 0)),
                        pl.BlockSpec((2, kv_rank, v_dim), lambda p, i: (pair(p, i), 0, 0)),
                    ] + [hbm] * (4 + len(cqs)) + [full] + [hbm] * len(deps),
                    out_specs=[pl.BlockSpec((rows, 2 * v_dim), lambda p, i: (0, p))] * 2,
                    scratch_shapes=[
                        pltpu.VMEM((groups, rows, kv_rank + 128), BF),
                        pltpu.VMEM((2, q_rank, rows), BF),
                        pltpu.VMEM((2, groups, rows, 256), BF),
                        pltpu.VMEM((groups, 2 * v_dim, rows), BF),
                        pltpu.VMEM((2, 2, 256, rows), BF),
                        pltpu.VMEM((groups, 2, rows, rows), F32),
                        pltpu.VMEM((2, 8, rows), F32),
                        pltpu.VMEM((2, 1, rows), F32),
                        pltpu.VMEM((2, 8, rows), F32),
                        pltpu.VMEM((2, v_dim, rows), F32),
                        pltpu.VMEM((2, 2, rows, v_dim), BF),
                        pltpu.SemaphoreType.DMA((6,)),
                    ],
                ),
                out_shape=[jax.ShapeDtypeStruct((rows, steps * 2 * v_dim), BF)] * 2,
                compiler_params=pltpu.CompilerParams(dimension_semantics=("arbitrary",), vmem_limit_bytes=48 << 20),
                cost_estimate=pl.CostEstimate(flops=5 * steps * 10 ** 9, bytes_accessed=2 * steps << 20, transcendentals=10 ** 7),
            )(info, wq_t, wk_h, wv_h, *lats, *cqs, cs, *deps)

        a_m, a_o = attend(6, 10, 7, 2, False)
        s_a = xor(a_o, 1)
        b_m, b_o = attend(moved, pairs - moved, 6, 0, True, a_m)
        r_m = xor(b_m, 2, (0, 1))
        r_o = xor(b_o, 3, (0, 1))
        s_b = xor(b_o, 1, (2, 3))
        c_m, c_o = attend(10, 0, pairs - 4, 4, False, b_m)
        s_c = xor(c_o, 1)
        early = ((2, 0, 10, 0), (0, 0, 6, 10))
        late = ((2, 4, 6, 0), (1, 0, 3, 6), (0, 2, 4, 9), (3, 0, 3, 13))
        bn = 512
        depth = own * v_dim
        info = jnp.stack([me, core]).astype(jnp.int32)
        w_o2 = w_o.reshape(heads * v_dim, width)
        attn_out = pl.pallas_call(
            lambda *r: out_kernel(early, late, *r),
            grid_spec=pltpu.PrefetchScalarGridSpec(
                num_scalar_prefetch=1,
                grid=(width // bn,),
                in_specs=[hbm] * 8 + [
                    pl.BlockSpec((depth, bn), lambda n, i: (i[1], n)),
                    pl.BlockSpec((depth, bn), lambda n, i: (1 - i[1], n))],
                out_specs=pl.BlockSpec((rows, bn), lambda n, i: (0, n)),
                scratch_shapes=[pltpu.VMEM((2, rows, depth), BF), pltpu.SemaphoreType.DMA((8,))],
            ),
            out_shape=jax.ShapeDtypeStruct((rows, width), BF),
            compiler_params=pltpu.CompilerParams(dimension_semantics=("arbitrary",), vmem_limit_bytes=56 << 20),
            cost_estimate=pl.CostEstimate(flops=52 * 10 ** 9, bytes_accessed=110 << 20, transcendentals=0),
            name="outproj",
        )(info, a_m, c_m, b_m, r_m, s_a, s_c, s_b, r_o, w_o2, w_o2)
        return attn_out, cache_kv, cache_pe

    return jax.shard_map(run, mesh=mesh, in_specs=(rows_spec, tok_spec) + (rep,) * 8, out_specs=(rows_spec,) * 3, check_vma=False)
```

```python
import math
import jax
import jax.numpy as jnp
from jax import lax
from jax.experimental import pallas as pl
from jax.experimental.pallas import tpu as pltpu
from jax.sharding import PartitionSpec as P

ROPE_THETA = 10000.0
YARN_FACTOR = 40.0
ORIG_CTX = 4096.0
BETA_FAST = 32.0
BETA_SLOW = 1.0
NORM_EPS = 1e-6
BF = jnp.bfloat16
F32 = jnp.float32


def rope_freqs(rot_dim):
    half_dim = rot_dim // 2
    log_base = 2.0 * math.log(ROPE_THETA)
    low_idx = max(math.floor(rot_dim * math.log(ORIG_CTX / (BETA_FAST * 2.0 * math.pi)) / log_base), 0)
    high_idx = min(math.ceil(rot_dim * math.log(ORIG_CTX / (BETA_SLOW * 2.0 * math.pi)) / log_base), half_dim - 1)
    spread = max(high_idx - low_idx, 0.001)
    freq_list = []
    for freq_idx in range(half_dim):
        base_freq = ROPE_THETA ** (-2.0 * freq_idx / rot_dim)
        ramp_val = min(max((freq_idx - low_idx) / spread, 0.0), 1.0)
        freq_list.append(base_freq / YARN_FACTOR * ramp_val + base_freq * (1.0 - ramp_val))
    return jnp.asarray(freq_list, dtype=F32)


def attn_kernel(scale, n_q, n_dep, info, *refs):
    wq, wk, wv = refs[:3]
    lats = refs[3:7]
    cqs = refs[7:7 + n_q]
    cs = refs[7 + n_q]
    o_m, o_o, ckv, cqv, kbuf, vbuf, qbuf, sbuf, m_ref, x_ref, l_ref, acc, obuf, sems = refs[8 + n_q + n_dep:]
    me, n_pieces, p_m, p_o, skip, q_slot = (info[k] for k in range(6))
    rows = cqv.shape[2]
    step = pl.program_id(0)

    @pl.when(step == 0)
    def _():
        def fetch(base):
            return [pltpu.make_async_copy(cqs[base + k], cqv.at[k], sems.at[k]) for k in range(2)]

        for base in range(0, n_q, 2):
            @pl.when(q_slot == base)
            def _():
                for c in fetch(base):
                    c.start()
        copies = [pltpu.make_async_copy(lats[k], ckv.at[jnp.bitwise_xor(me, k)], sems.at[2 + k]) for k in range(4)]
        for c in copies:
            c.start()
        for c in copies + fetch(0):
            c.wait()
        qbuf[:, :, 192:, :] = jnp.zeros_like(qbuf[:, :, 192:, :])

        @pl.loop(0, n_pieces)
        def _(c):
            for h in range(2):
                kbuf[h, c, :, 128:] = ckv[c, :, 512:]

    @pl.when(step >= skip)
    def _():
        @pl.loop(0, 2)
        def _(k):
            t = cs[q_slot + k]
            cos, sin = t[:32], t[32:]
            u = jnp.dot(wq[...], cqv[k], preferred_element_type=F32)
            for h in range(2):
                b = 192 * h
                z1, z2 = u[b + 128:b + 160], u[b + 160:b + 192]
                qbuf[k, h, 0:128] = u[b:b + 128].astype(BF)
                qbuf[k, h, 128:160] = (z1 * cos - z2 * sin).astype(BF)
                qbuf[k, h, 160:192] = (z2 * cos + z1 * sin).astype(BF)

        wkv = jnp.concatenate([wk[0], wk[1], wv[0], wv[1]], axis=1)

        @pl.loop(0, n_pieces)
        def _(c):
            kv = jnp.dot(ckv[c, :, :512], wkv, preferred_element_type=F32).astype(BF)
            kbuf[0, c, :, :128] = kv[:, :128]
            kbuf[1, c, :, :128] = kv[:, 128:256]
            vbuf[c] = kv[:, 256:].T

        @pl.loop(0, 2)
        def _(st):
            p_st = jnp.where(st == 0, p_m, p_o)
            m_ref[...] = jnp.full_like(m_ref, -jnp.inf)
            l_ref[...] = jnp.zeros_like(l_ref)
            acc[...] = jnp.zeros_like(acc)

            def first(c, h, masked):
                s = jnp.dot(kbuf[h, c], qbuf[st, h], preferred_element_type=F32)
                if masked:
                    keep = lax.broadcasted_iota(jnp.int32, (rows, rows), 0) <= lax.broadcasted_iota(jnp.int32, (rows, rows), 1)
                    s = jnp.where(keep, s, -jnp.inf)
                sbuf[c, h] = s
                m_ref[h] = jnp.maximum(m_ref[h], jnp.max(s.reshape(rows // 8, 8, rows), axis=0))

            def second(c, h):
                m = x_ref[h]
                p = jnp.exp2((sbuf[c, h] - m) * scale)
                l_ref[h] = l_ref[h] + jnp.sum(p.reshape(rows // 8, 8, rows), axis=0)
                acc[h] = acc[h] + jnp.dot(vbuf[c, pl.ds(128 * h, 128)], p.astype(BF), preferred_element_type=F32)

            def both(f):
                f(0)
                f(1)

            @pl.loop(0, p_st)
            def _(c):
                both(lambda h: first(c, h, False))

            both(lambda h: first(p_st, h, True))
            for h in range(2):
                x_ref[h] = jnp.max(m_ref[h], axis=0, keepdims=True)

            @pl.loop(0, p_st + 1)
            def _(c):
                both(lambda h: second(c, h))

            for h in range(2):
                total = jnp.sum(l_ref[h], axis=0, keepdims=True)
                obuf[st, h] = (acc[h] * (1.0 / total)).astype(BF).T

        for st, out in ((0, o_m), (1, o_o)):
            for h in range(2):
                out[:, 128 * h:128 * h + 128] = obuf[st, h]


def head_major(info, a, b, out_a, out_b):
    out_a[...] = jnp.swapaxes(a[...], 0, 1)
    out_b[...] = jnp.swapaxes(b[...], 0, 1)


def out_kernel(early, late, info, a_m, c_m, b_m, r_m, a_o, c_o, b_o, r_o, wa, wb, y, buf, sems):
    col = 256

    @pl.when(pl.program_id(0) == 0)
    def _():
        for is_late, runs in ((False, early), (True, late)):
            @pl.when((info[0] >= 2) == is_late)
            def _():
                copies = []
                for g, part in enumerate(((a_m, b_m, c_m, r_m), (a_o, b_o, c_o, r_o))):
                    for n, (src, first, count, place) in enumerate(runs):
                        copies.append(pltpu.make_async_copy(
                            part[src].at[:, pl.ds(first * col, count * col)],
                            buf.at[g, :, pl.ds(place * col, count * col)], sems.at[4 * g + n]))
                for c in copies:
                    c.start()
                for c in copies:
                    c.wait()

    r = jnp.dot(buf[0], wa[...], preferred_element_type=F32) + jnp.dot(buf[1], wb[...], preferred_element_type=F32)
    y[...] = r.astype(BF)


def solution(mesh):
    groups = mesh.shape['sp']
    tok_spec = P(('dp', 'sp'))
    rows_spec = P(('dp', 'sp'), None)
    rep = P()

    def xor(x, k, sources=range(4)):
        return lax.ppermute(x, 'sp', [(i, i ^ k) for i in sources])

    def run(tok_in, tok_pos, w_dq, g_q, w_uq, w_dkv, g_kv, w_uk, w_uv, w_o):
        rows, width = tok_in.shape
        heads, qk_dim = w_uq.shape[1], w_uq.shape[2]
        q_rank, kv_rank = w_dq.shape[1], g_kv.shape[0]
        v_dim = w_uv.shape[2]
        rot = w_dkv.shape[1] - kv_rank
        half = rot // 2
        own = heads // 2
        pairs = own // 2
        moved = 3
        scale = (0.1 * math.log(YARN_FACTOR) + 1.0) ** 2 / math.sqrt(qk_dim) * math.log2(math.e)
        me = lax.axis_index('sp')
        core = jnp.bitwise_and(me, 1)
        is_late = me >= 2

        pos = jnp.stack([tok_pos] + [xor(tok_pos, k) for k in range(1, 4)])
        angles = pos.astype(F32)[:, None, :] * rope_freqs(rot)[None, :, None]
        cs = jnp.concatenate([jnp.cos(angles), jnp.sin(angles)], axis=1)
        my_angles = tok_pos.astype(F32)[:, None] * rope_freqs(rot)[None, :]
        cos_t, sin_t = jnp.cos(my_angles), jnp.sin(my_angles)
        kv = jnp.dot(tok_in, w_dkv, preferred_element_type=F32)
        a, b1, b2 = kv[:, :kv_rank], kv[:, kv_rank:kv_rank + half], kv[:, kv_rank + half:]
        cache_kv = (a * lax.rsqrt(jnp.mean(a * a, axis=-1, keepdims=True) + NORM_EPS) * g_kv).astype(BF)
        cache_pe = jnp.concatenate([b1 * cos_t - b2 * sin_t, b2 * cos_t + b1 * sin_t], axis=-1).astype(BF)
        lat = jnp.concatenate([cache_kv, cache_pe, jnp.zeros((rows, 128 - rot), BF)], axis=1)
        lat_x = xor(lat, 2)
        lats = [lat, xor(lat, 1), lat_x, xor(lat_x, 1)]

        tok_in, lat = lax.optimization_barrier((tok_in, lat))
        uq = jnp.dot(tok_in, w_dq, preferred_element_type=F32)
        inv = lax.rsqrt(jnp.mean(uq * uq, axis=-1, keepdims=True) + NORM_EPS)
        c_q = (uq * inv * g_q).astype(BF).T
        cq_o = xor(c_q, 1)
        cq_x = xor(c_q, 2, (2, 3))
        cq_y = xor(cq_x, 1, (0, 1))

        wq_t = jnp.transpose(w_uq, (1, 2, 0)).reshape(heads * qk_dim, q_rank)
        blocks = own // 8
        wk_h, wv_h = pl.pallas_call(
            head_major,
            grid_spec=pltpu.PrefetchScalarGridSpec(
                num_scalar_prefetch=1,
                grid=(blocks,),
                in_specs=[pl.BlockSpec((kv_rank, 8, v_dim), lambda g, i: (0, i[0] * blocks + g, 0))] * 2,
                out_specs=[pl.BlockSpec((8, kv_rank, v_dim), lambda g, i: (g, 0, 0))] * 2,
            ),
            out_shape=[jax.ShapeDtypeStruct((own, kv_rank, v_dim), BF)] * 2,
            compiler_params=pltpu.CompilerParams(dimension_semantics=("arbitrary",), vmem_limit_bytes=32 << 20),
            cost_estimate=pl.CostEstimate(flops=10 ** 8, bytes_accessed=16 << 20, transcendentals=0),
            name="headmajor",
        )(core[None], w_uk, w_uv)
        full = pl.BlockSpec(memory_space=pltpu.VMEM)
        hbm = pl.BlockSpec(memory_space=pl.ANY)

        def attend(steps, early_pair, late_pair, late_skip, foreign, *deps):
            pair0 = jnp.where(is_late, late_pair, early_pair)
            skip = jnp.where(is_late, late_skip, 0)
            if foreign:
                base = jnp.where(is_late, me, me ^ 2)
                pieces = jnp.full((), 4, jnp.int32)
                slot = jnp.where(is_late, 0, 2)
                cqs = [c_q, cq_o, cq_x, cq_y]
            else:
                base, pieces, slot = me, jnp.where(is_late, 4, 2), jnp.zeros((), jnp.int32)
                cqs = [c_q, cq_o]
            info = jnp.stack([me, pieces, base, base ^ 1, skip, slot, pair0, core]).astype(jnp.int32)

            def pair(p, i):
                return jnp.bitwise_and(i[6] + jnp.maximum(p, i[4]), pairs - 1)

            return pl.pallas_call(
                lambda *r: attn_kernel(scale, len(cqs), len(deps), *r),
                grid_spec=pltpu.PrefetchScalarGridSpec(
                    num_scalar_prefetch=1,
                    grid=(steps,),
                    in_specs=[
                        pl.BlockSpec((2 * qk_dim, q_rank), lambda p, i: (i[7] * pairs + pair(p, i), 0)),
                        pl.BlockSpec((2, kv_rank, v_dim), lambda p, i: (pair(p, i), 0, 0)),
                        pl.BlockSpec((2, kv_rank, v_dim), lambda p, i: (pair(p, i), 0, 0)),
                    ] + [hbm] * (4 + len(cqs)) + [full] + [hbm] * len(deps),
                    out_specs=[pl.BlockSpec((rows, 2 * v_dim), lambda p, i: (0, p))] * 2,
                    scratch_shapes=[
                        pltpu.VMEM((groups, rows, kv_rank + 128), BF),
                        pltpu.VMEM((2, q_rank, rows), BF),
                        pltpu.VMEM((2, groups, rows, 256), BF),
                        pltpu.VMEM((groups, 2 * v_dim, rows), BF),
                        pltpu.VMEM((2, 2, 256, rows), BF),
                        pltpu.VMEM((groups, 2, rows, rows), F32),
                        pltpu.VMEM((2, 8, rows), F32),
                        pltpu.VMEM((2, 1, rows), F32),
                        pltpu.VMEM((2, 8, rows), F32),
                        pltpu.VMEM((2, v_dim, rows), F32),
                        pltpu.VMEM((2, 2, rows, v_dim), BF),
                        pltpu.SemaphoreType.DMA((6,)),
                    ],
                ),
                out_shape=[jax.ShapeDtypeStruct((rows, steps * 2 * v_dim), BF)] * 2,
                compiler_params=pltpu.CompilerParams(dimension_semantics=("arbitrary",), vmem_limit_bytes=48 << 20),
                cost_estimate=pl.CostEstimate(flops=5 * steps * 10 ** 9, bytes_accessed=2 * steps << 20, transcendentals=10 ** 7),
            )(info, wq_t, wk_h, wv_h, *lats, *cqs, cs, *deps)

        a_m, a_o = attend(6, 10, 7, 2, False)
        s_a = xor(a_o, 1)
        b_m, b_o = attend(moved, pairs - moved, 6, 0, True, a_m)
        r_m = xor(b_m, 2, (0, 1))
        r_o = xor(b_o, 3, (0, 1))
        s_b = xor(b_o, 1, (2, 3))
        c_m, c_o = attend(10, 0, pairs - 4, 4, False, b_m)
        s_c = xor(c_o, 1)
        early = ((2, 0, 10, 0), (0, 0, 6, 10))
        late = ((2, 4, 6, 0), (1, 0, 3, 6), (0, 2, 4, 9), (3, 0, 3, 13))
        bn = 512
        depth = own * v_dim
        info = jnp.stack([me, core]).astype(jnp.int32)
        w_o2 = w_o.reshape(heads * v_dim, width)
        attn_out = pl.pallas_call(
            lambda *r: out_kernel(early, late, *r),
            grid_spec=pltpu.PrefetchScalarGridSpec(
                num_scalar_prefetch=1,
                grid=(width // bn,),
                in_specs=[hbm] * 8 + [
                    pl.BlockSpec((depth, bn), lambda n, i: (i[1], n)),
                    pl.BlockSpec((depth, bn), lambda n, i: (1 - i[1], n))],
                out_specs=pl.BlockSpec((rows, bn), lambda n, i: (0, n)),
                scratch_shapes=[pltpu.VMEM((2, rows, depth), BF), pltpu.SemaphoreType.DMA((8,))],
            ),
            out_shape=jax.ShapeDtypeStruct((rows, width), BF),
            compiler_params=pltpu.CompilerParams(dimension_semantics=("arbitrary",), vmem_limit_bytes=56 << 20),
            cost_estimate=pl.CostEstimate(flops=52 * 10 ** 9, bytes_accessed=110 << 20, transcendentals=0),
            name="outproj",
        )(info, a_m, c_m, b_m, r_m, s_a, s_c, s_b, r_o, w_o2, w_o2)
        return attn_out, cache_kv, cache_pe

    return jax.shard_map(run, mesh=mesh, in_specs=(rows_spec, tok_spec) + (rep,) * 8, out_specs=(rows_spec,) * 3, check_vma=False)
```
